512 devices in a mesh: grp: 2 (over y), gz: 16 (over z), gy: 8 (over x), sa: 2 (over core).
Axes of the slice: x: 8, y: 2, z: 16, core: 2. Of those that a mesh axis runs over, the one named last changes fastest.
The devices are a block of a 8x8x16 slice.
Arguments:
- field: float32 [8, 128, 64, 128], P('sa', ('grp', 'gz'), 'gy'), parts along dimension 1, may hold values from 0 to 2
- diffusion: float32 [8], P('sa'), may hold values from 0.02 to 0.16
- secrete: float32 [8, 1048576], P('sa', ('grp', 'gz', 'gy')), parts along dimension 1, may hold values from 0 to 1
- uptake: float32 [8, 1048576], P('sa', ('grp', 'gz', 'gy')), parts along dimension 1, may hold values from 0.05 to 1
- cell_voxel: int32 [1048576], P(('grp', 'gz', 'gy')), parts along dimension 0, may hold values from 0 to 4095
- block_dest: int32 [8192, 1], P(('grp', 'gz', 'gy')), parts along dimension 0, may hold values from 0 to 15; in each aligned block of 32 rows (0 to 31, 32 to 63, ...) at most 6 rows name the same one
Outputs:
- new_field: float32 [8, 128, 64, 128], P('sa', ('grp', 'gz'), 'gy'), parts along dimension 1
- cell_conc: float32 [8, 1048576], P('sa', ('grp', 'gz', 'gy')), parts along dimension 1
The draws below stay inside these ranges and needn't reach their ends.
There are 2 independent parts, one for each index of `grp`. The reference program is written for one: setup_inputs(seed, part) draws one part's arguments, and reference() takes and returns one part's arrays. A program takes and returns all parts, laid end to end along the dimension named above; an argument that names none is the same for every part. Nothing has to cross between parts.
Inputs may be any that keep to these rules, and one draw needn't show every extreme that they name: `block_dest`: among the 32 blocks of one device at most 6 name the same destination, and in every draw some device has exactly 6 blocks naming one destination.
All inputs are finite; a program needn't handle non-finite values.
Results may differ from the reference program's by a relative error of at most 0.00007.
Values sent between devices are 32-bit elements; how exact they have to be, the bound alone decides.
No kernel may reach another device: no remote copies, remote signals or barrier semaphores. Data moves between devices by JAX's collectives and lax.ppermute only.
A program may use at most 64 MiB of HBM per device.

```python
import math
import jax
import jax.numpy as jnp
import numpy as np

SUBS = 8
BLOCK_CELLS = 128
BLK_DEV = 32
VZ = 4
VY = 8
NXV = 128
VOX = 4096
NZ = 64
NY = 64
CELLS = 524288
BLOCKS = 4096
CAP = 6
N_GZ = 16
N_GY = 8


def plant(drawn, rng, low, largest):
    dims = drawn.shape
    spot = [jax.random.randint(jax.random.fold_in(rng, axis), (), 0, dims[axis]) for axis in range(len(dims))]
    drawn = drawn.at[tuple(spot)].set(low)
    longest = dims.index(max(dims))
    spot[longest] = (spot[longest] + 1) % dims[longest]
    return drawn.at[tuple(spot)].set(largest)


def steps_of(own_key, shape, pieces, smallest, top_value):
    factor_of, own = 1.0, jax.random.fold_in(own_key, 6)
    for axis_at, shards_of in pieces:
        steps = jnp.exp(jax.random.uniform(jax.random.fold_in(own, axis_at), (shards_of,), jnp.float32, smallest / len(pieces), top_value / len(pieces)))
        factor_of = factor_of * jnp.repeat(steps, shape[axis_at] // shards_of).reshape([-1 if axis == axis_at else 1 for axis in range(len(shape))])
    return factor_of


def deal_out(rng, own, number, rows, amount, top, most, lean):
    sequence = jax.random.permutation(rng, amount)
    crowded, ordinary = portions_of(amount, rows * top, most, lean, True), portions_of(amount, rows * top, most, lean, False)
    places = jnp.arange(amount)

    def named(tallies, turn):
        used = int((tallies > 0).sum())
        fixed = max(1, used // 4)
        moved = fixed + (places - fixed + turn * (used - fixed)) % max(1, amount - fixed)
        return jnp.zeros((amount,), jnp.int32).at[sequence[jnp.where(places < fixed, places, moved)]].set(jnp.asarray(tallies, jnp.int32))

    tallies = jnp.where(number % 4 == 0, named(crowded, number // 4), named(ordinary, number - number // 4 - 1))
    mixed = jax.random.permutation(jax.random.fold_in(own, 3), amount)
    giver, sink = mixed[0:amount // 2 * 2:2], mixed[1:amount // 2 * 2:2]
    room = jnp.minimum(tallies[giver] - 1, most - tallies[sink]) // 2
    room = jnp.where((giver == sequence[0]) | (sink == sequence[0]) | (tallies[sink] == 0), 0, jnp.maximum(room, 0))
    moved = jax.random.randint(jax.random.fold_in(own, 4), (amount // 2,), 0, 1 << 20) % (room + 1)
    tallies = tallies.at[giver].add(-moved).at[sink].add(moved)
    members = jnp.searchsorted(jnp.cumsum(tallies), jnp.arange(rows * top), side="right").astype(jnp.int32)
    table = members.reshape(top, rows).T
    table = table[jax.random.permutation(jax.random.fold_in(own, 1), rows)]
    turn = jax.random.randint(jax.random.fold_in(own, 2), (rows, 1), 0, top)
    return jnp.take_along_axis(table, (jnp.arange(top)[None, :] + turn) % top, axis=1)


def portions_of(amount, total, limit, skew, full):
    loads = [(1 << 20) // math.isqrt(grade ** skew) + 1 for grade in range(1, amount + 1)]
    largest = limit if full else min(limit, max(-(-total // amount), total * loads[0] // sum(loads)))
    least = 1 if total - largest >= amount - 1 else 0
    given, rest = [largest] + [least] * (amount - 1), total - largest - least * (amount - 1)
    while rest > 0:
        candidates = [i for i in range(1, amount) if given[i] < largest] or [i for i in range(1, amount) if given[i] < limit]
        pool, left = sum([loads[i] for i in candidates]), rest
        for i in candidates:
            extra = min(limit - given[i], max(1, left * loads[i] // pool), rest)
            given[i] = given[i] + extra
            rest = rest - extra
    return np.array(given)


def setup_inputs(seed: int = 0, part: int = 0) -> dict:
    seeds = jax.random.split(jax.random.key(seed), 7)
    part_splits = jax.random.split(jax.random.fold_in(seeds[6], part), 7)
    field = jnp.clip(2.0 * jax.random.uniform(part_splits[0], (SUBS, NZ, NY, NXV), jnp.float32) ** steps_of(part_splits[0], (SUBS, NZ, NY, NXV), ((0, 2), (1, 16), (2, 8)), -0.2, 0.2), 0.0, 2.0)
    diffusion = jnp.clip(jnp.exp(math.log(0.16) - 2.0794415 * jax.random.uniform(seeds[1], (SUBS,), jnp.float32) ** steps_of(seeds[1], (SUBS,), ((0, 2),), -0.2, 0.2)), 0.02, 0.16)
    secrete = jnp.clip(1.0 * jax.random.uniform(part_splits[2], (SUBS, CELLS), jnp.float32) ** steps_of(part_splits[2], (SUBS, CELLS), ((0, 2), (1, 128)), -0.2, 0.2), 0.0, 1.0)
    uptake = jnp.clip(jnp.exp(math.log(1.0) - 2.9957323 * jax.random.uniform(part_splits[3], (SUBS, CELLS), jnp.float32) ** steps_of(part_splits[3], (SUBS, CELLS), ((0, 2), (1, 128)), -0.2, 0.2)), 0.05, 1.0)
    cell_voxel = plant(jax.random.randint(part_splits[4], (CELLS,), 0, VOX), jax.random.fold_in(part_splits[4], 1), 0, VOX - 1).astype(jnp.int32)
    block_dest_keys = jax.random.split(jax.random.fold_in(part_splits[5], 1), BLOCKS // BLK_DEV)
    block_dest_turns = jax.random.permutation(jax.random.fold_in(part_splits[5], 3), BLOCKS // BLK_DEV)
    block_dest = jax.vmap(lambda own, number: deal_out(jax.random.fold_in(part_splits[5], 2), own, number, BLK_DEV, N_GZ, 1, CAP, 2))(block_dest_keys, block_dest_turns).reshape((BLOCKS, 1))
    return dict(field=field, diffusion=diffusion, secrete=secrete, uptake=uptake, cell_voxel=cell_voxel, block_dest=block_dest)


def neighbours(padded):
    beside_all = padded[:, 2:, 1:-1, 1:-1] + padded[:, :-2, 1:-1, 1:-1]
    beside_all = beside_all + padded[:, 1:-1, 2:, 1:-1] + padded[:, 1:-1, :-2, 1:-1]
    return beside_all + padded[:, 1:-1, 1:-1, 2:] + padded[:, 1:-1, 1:-1, :-2]


def reference(field, diffusion, secrete, uptake, cell_voxel, block_dest):
    padded = jnp.pad(field, ((0, 0), (1, 1), (1, 1), (1, 1)))
    diffused = field + diffusion[:, None, None, None] * (neighbours(padded) - 6.0 * field)
    substrates = field.shape[0]
    cells_total = cell_voxel.shape[0]
    per_device = cells_total // (N_GZ * N_GY)
    cell_index = jnp.arange(cells_total, dtype=jnp.int32)
    home_device = cell_index // per_device
    home_row = home_device % N_GY
    cell_dest = jnp.repeat(block_dest[:, 0], BLOCK_CELLS, total_repeat_length=cells_total)
    voxel_z = cell_voxel // (VY * NXV)
    voxel_y = (cell_voxel // NXV) % VY
    voxel_x = cell_voxel % NXV
    global_z = cell_dest * VZ + voxel_z
    global_y = home_row * VY + voxel_y
    flat_index = ((global_z * NY + global_y) * NXV + voxel_x).astype(jnp.int32)
    total_voxels = NZ * NY * NXV
    source = jnp.zeros((substrates, total_voxels), jnp.float32).at[:, flat_index].add(secrete)
    uptake_sum = jnp.zeros((substrates, total_voxels), jnp.float32).at[:, flat_index].add(uptake)
    updated = (diffused.reshape(substrates, total_voxels) + source) / (1.0 + uptake_sum)
    cell_conc = updated[:, flat_index]
    return updated.reshape(field.shape), cell_conc
```

```python
import functools

import jax
import jax.numpy as jnp
from jax import lax
from jax.experimental import pallas as pl
from jax.experimental.pallas import tpu as pltpu
from jax.sharding import PartitionSpec as P

CAP = 6


def extended(x, sides, width):
    edges = {}
    for axis, dim in sides:
        size, length = (lax.axis_size(axis), x.shape[dim])
        up = [(i, (i + 1) % size) for i in range(size - 1)]
        last = lax.slice_in_dim(x, length - width, length, axis=dim)
        leading = lax.slice_in_dim(x, 0, width, axis=dim)
        edges[dim] = (
            lax.ppermute(last, axis, up),
            lax.ppermute(leading, axis, [(b, a) for a, b in up]),
        )
    done = []
    for _, dim in sides:
        low, high = edges[dim]
        around = [(width, width) if d in done else (0, 0) for d in range(x.ndim)]
        x = jnp.concatenate([jnp.pad(low, around), x, jnp.pad(high, around)], axis=dim)
        done.append(dim)
    return x


def neighbours(padded):
    beside_all = padded[:, 2:, 1:-1, 1:-1] + padded[:, :-2, 1:-1, 1:-1]
    beside_all = beside_all + padded[:, 1:-1, 2:, 1:-1] + padded[:, 1:-1, :-2, 1:-1]
    return beside_all + padded[:, 1:-1, 1:-1, 2:] + padded[:, 1:-1, 1:-1, :-2]


def diffuse(field, diffusion):
    padded = extended(field, (("gz", 1), ("gy", 2)), 1)
    padded = jnp.pad(padded, ((0, 0), (0, 0), (0, 0), (1, 1)))
    return field + diffusion[:, None, None, None] * (neighbours(padded) - 6.0 * field)


def rows_of(channels):
    return CAP * channels, -(-(CAP * channels + CAP) // 8) * 8


def pack_kernel(dest, secrete, uptake, voxel, out, used, *, blocks, cells, subs):
    slabs = out.shape[0]
    base, rows = rows_of(2 * subs)
    out[:, pl.ds(0, base), :] = jnp.zeros((slabs, base, cells), jnp.float32)
    out[:, pl.ds(base, rows - base), :] = jnp.full((slabs, rows - base, cells), -1.0, jnp.float32)
    for i in range(slabs):
        used[i] = 0
    for b in range(blocks):
        to = dest[b]
        slot = used[to]
        used[to] = slot + 1
        at = slice(b * cells, (b + 1) * cells)
        out[to, pl.ds(slot * 2 * subs, subs), :] = secrete[:, at]
        out[to, pl.ds(slot * 2 * subs + subs, subs), :] = uptake[:, at]
        out[to, pl.ds(base + slot, 1), :] = voxel[b : b + 1, :].astype(jnp.float32)


def place_kernel(dest, came, out, used, *, blocks, cells, subs):
    for i in range(came.shape[0]):
        used[i] = 0
    for b in range(blocks):
        to = dest[b]
        slot = used[to]
        used[to] = slot + 1
        out[:, b * cells : (b + 1) * cells] = came[to, pl.ds(slot * subs, subs), :]


def halves(x):
    high = x.astype(jnp.bfloat16)
    return high, (x - high.astype(jnp.float32)).astype(jnp.bfloat16)


def cells_of_pair(got, i, j, base, highs, lanes):
    v = jnp.concatenate(
        [got[i, pl.ds(base + 2 * j, 1), :], got[i, pl.ds(base + 2 * j + 1, 1), :]], axis=1
    ).astype(jnp.int32)
    row = v // lanes
    high = jnp.where(v < 0, -1, row % highs)
    low = v % lanes + lanes * (row // highs)
    wide = 2 * lanes
    mask = lax.broadcasted_iota(jnp.int32, (highs, wide), 0) == high
    lows = jnp.broadcast_to(low.astype(jnp.float32), (wide, wide)).astype(jnp.bfloat16)
    ids = lax.broadcasted_iota(jnp.int32, (wide, wide), 0).astype(jnp.float32).astype(jnp.bfloat16)
    one, zero = jnp.bfloat16(1.0), jnp.bfloat16(0.0)
    return mask, jnp.where(ids == lows, one, zero)


def cell_kernel(got, diffused, new_field, back, acc, table, *, subs):
    slabs, _, lanes = got.shape
    channels = 2 * subs
    base, _ = rows_of(channels)
    highs = diffused.shape[1] // 2
    wide = 2 * lanes
    pairs = CAP // 2
    acc[...] = jnp.zeros(acc.shape, jnp.float32)

    def add(i, unused):
        for j in range(pairs):
            mask, onehot = cells_of_pair(got, i, j, base, highs, lanes)
            two = [got[i, pl.ds((2 * j + k) * channels, channels), :] for k in range(2)]
            high, low = halves(jnp.concatenate(two, axis=1))
            values = jnp.concatenate([high.astype(jnp.float32), low.astype(jnp.float32)], axis=0)
            spread = jnp.where(mask[None], values[:, None, :], 0.0).astype(jnp.bfloat16)
            spread = spread.reshape(2 * channels * highs, wide)
            acc[...] += lax.dot_general(
                spread, onehot, (((1,), (1,)), ((), ())), preferred_element_type=jnp.float32
            )
        return unused

    lax.fori_loop(0, slabs, add, 0)
    half = channels * highs
    sums = (acc[0:half, :] + acc[half : 2 * half, :]).reshape(channels, highs, wide)
    sums = jnp.concatenate([sums[:, :, :lanes], sums[:, :, lanes:]], axis=1)
    new = (diffused[...] + sums[:subs]) / (1.0 + sums[subs:])
    new_field[...] = new
    by_low = jnp.concatenate([new[:, :highs], new[:, highs:]], axis=2).reshape(subs * highs, wide)
    part = halves(by_low)
    table[...] = jnp.concatenate(part, axis=0)

    def read(i, unused):
        for j in range(pairs):
            mask, onehot = cells_of_pair(got, i, j, base, highs, lanes)
            rows = jnp.dot(table[...], onehot, preferred_element_type=jnp.float32)
            rows = (rows[: subs * highs] + rows[subs * highs :]).reshape(subs, highs, wide)
            found = jnp.sum(jnp.where(mask[None], rows, 0.0), axis=1)
            for k in range(2):
                back[i, pl.ds((2 * j + k) * subs, subs), :] = found[:, k * lanes : (k + 1) * lanes]
        return unused

    lax.fori_loop(0, slabs, read, 0)


def small(mebibytes):
    return pltpu.CompilerParams(vmem_limit_bytes=mebibytes << 20)


def vmem():
    return pl.BlockSpec(memory_space=pltpu.VMEM)


def smem():
    return pl.BlockSpec(memory_space=pltpu.SMEM)


def shards(field, diffusion, secrete, uptake, cell_voxel, block_dest):
    subs, lanes = field.shape[0], field.shape[3]
    lines = field.shape[1] * field.shape[2]
    blocks = block_dest.shape[0]
    cells = secrete.shape[1] // blocks
    slabs = lax.axis_size("gz")
    base, rows = rows_of(2 * subs)
    f32 = functools.partial(jax.ShapeDtypeStruct, dtype=jnp.float32)
    dest = block_dest.reshape(blocks)
    sent = pl.pallas_call(
        functools.partial(pack_kernel, blocks=blocks, cells=cells, subs=subs),
        out_shape=f32((slabs, rows, cells)),
        in_specs=[smem(), vmem(), vmem(), vmem()],
        out_specs=vmem(),
        scratch_shapes=[pltpu.SMEM((slabs,), jnp.int32)],
        compiler_params=small(4),
        name="pack",
    )(dest, secrete, uptake, cell_voxel.reshape(blocks, cells))
    got = lax.all_to_all(sent, "gz", split_axis=0, concat_axis=0, tiled=True)
    diffused = diffuse(field, diffusion).reshape(subs, lines, lanes)
    new_field, back = pl.pallas_call(
        functools.partial(cell_kernel, subs=subs),
        out_shape=(f32((subs, lines, lanes)), f32((slabs, CAP * subs, cells))),
        in_specs=[vmem(), vmem()],
        out_specs=(vmem(), vmem()),
        scratch_shapes=[
            pltpu.VMEM((4 * subs * lines // 2, 2 * lanes), jnp.float32),
            pltpu.VMEM((2 * subs * lines // 2, 2 * lanes), jnp.bfloat16),
        ],
        compiler_params=small(8),
        name="cells",
    )(got, diffused)
    came = lax.all_to_all(back, "gz", split_axis=0, concat_axis=0, tiled=True)
    cell_conc = pl.pallas_call(
        functools.partial(place_kernel, blocks=blocks, cells=cells, subs=subs),
        out_shape=f32((subs, blocks * cells)),
        in_specs=[smem(), vmem()],
        out_specs=vmem(),
        scratch_shapes=[pltpu.SMEM((slabs,), jnp.int32)],
        compiler_params=small(4),
        name="place",
    )(dest, came)
    return (new_field.reshape(field.shape), cell_conc)


def solution(mesh):
    in_specs = (
        P("sa", ("grp", "gz"), "gy", None),
        P("sa"),
        P("sa", ("grp", "gz", "gy")),
        P("sa", ("grp", "gz", "gy")),
        P(("grp", "gz", "gy")),
        P(("grp", "gz", "gy"), None),
    )
    out_specs = (P("sa", ("grp", "gz"), "gy", None), P("sa", ("grp", "gz", "gy")))
    return jax.shard_map(shards, mesh=mesh, in_specs=in_specs, out_specs=out_specs, check_vma=False)
```

```python
import functools

import jax
import jax.numpy as jnp
from jax import lax
from jax.experimental import pallas as pl
from jax.experimental.pallas import tpu as pltpu
from jax.sharding import PartitionSpec as P

CAP = 6


def extended(x, sides, width):
    edges = {}
    for axis, dim in sides:
        size, length = (lax.axis_size(axis), x.shape[dim])
        up = [(i, (i + 1) % size) for i in range(size - 1)]
        last = lax.slice_in_dim(x, length - width, length, axis=dim)
        leading = lax.slice_in_dim(x, 0, width, axis=dim)
        edges[dim] = (
            lax.ppermute(last, axis, up),
            lax.ppermute(leading, axis, [(b, a) for a, b in up]),
        )
    done = []
    for _, dim in sides:
        low, high = edges[dim]
        around = [(width, width) if d in done else (0, 0) for d in range(x.ndim)]
        x = jnp.concatenate([jnp.pad(low, around), x, jnp.pad(high, around)], axis=dim)
        done.append(dim)
    return x


def neighbours(padded):
    beside_all = padded[:, 2:, 1:-1, 1:-1] + padded[:, :-2, 1:-1, 1:-1]
    beside_all = beside_all + padded[:, 1:-1, 2:, 1:-1] + padded[:, 1:-1, :-2, 1:-1]
    return beside_all + padded[:, 1:-1, 1:-1, 2:] + padded[:, 1:-1, 1:-1, :-2]


def diffuse(field, diffusion):
    padded = extended(field, (("gz", 1), ("gy", 2)), 1)
    padded = jnp.pad(padded, ((0, 0), (0, 0), (0, 0), (1, 1)))
    return field + diffusion[:, None, None, None] * (neighbours(padded) - 6.0 * field)


def rows_of(channels):
    return CAP * channels, -(-(CAP * channels + CAP) // 8) * 8


def pack_kernel(
    dest_in, secrete_in, uptake_in, voxel_in, out, dest, secrete, uptake, voxel, used, sems, *, subs
):
    pairs = ((dest_in, dest), (secrete_in, secrete), (uptake_in, uptake), (voxel_in, voxel))
    copies = [pltpu.make_async_copy(a, b, sems.at[i]) for i, (a, b) in enumerate(pairs)]
    for copy in copies:
        copy.start()
    slabs, _, cells = out.shape
    base, rows = rows_of(2 * subs)
    out[:, pl.ds(base, rows - base), :] = jnp.full((slabs, rows - base, cells), -1.0, jnp.float32)
    for i in range(slabs):
        used[i] = 0
    for copy in copies:
        copy.wait()
    for b in range(dest.shape[0]):
        to = dest[b]
        slot = used[to]
        used[to] = slot + 1
        at = slice(b * cells, (b + 1) * cells)
        out[to, pl.ds(slot * 2 * subs, subs), :] = secrete[:, at]
        out[to, pl.ds(slot * 2 * subs + subs, subs), :] = uptake[:, at]
        out[to, pl.ds(base + slot, 1), :] = voxel[b : b + 1, :].astype(jnp.float32)
    for i in range(slabs):
        out[i, base + CAP : base + CAP + 1, :] = jnp.full((1, cells), used[i]).astype(jnp.float32)


def place_kernel(dest, came, out, used, *, blocks, cells, subs):
    for i in range(came.shape[0]):
        used[i] = 0
    for b in range(blocks):
        to = dest[b]
        slot = used[to]
        used[to] = slot + 1
        out[:, b * cells : (b + 1) * cells] = came[to, pl.ds(slot * subs, subs), :]


def halves(x):
    high = x.astype(jnp.bfloat16)
    return high, (x - high.astype(jnp.float32)).astype(jnp.bfloat16)


GROUP = 4
BITS = 10


def list_blocks(got, work, slabs, subs):
    base, rows = rows_of(2 * subs)
    counts = jnp.concatenate([got[i * rows + base + CAP : i * rows + base + CAP + 1, :] for i in range(slabs)], axis=0)
    lane = lax.broadcasted_iota(jnp.int32, (8, counts.shape[1]), 1)
    digit = lax.broadcasted_iota(jnp.int32, (8, counts.shape[1]), 0)
    scale = jnp.where(lane == 0, 1 << (3 * digit), 0).astype(jnp.float32)
    words = [jnp.sum(counts[8 * w : 8 * w + 8] * scale).astype(jnp.int32) for w in range(slabs // 8)]
    total, hole = jnp.int32(0), jnp.int32(0)
    for i in range(slabs):
        count = (words[i // 8] >> (3 * (i % 8))) & 7
        for slot in range(CAP):
            at = i * rows + slot * 2 * subs, i * rows + base + slot, i * CAP * subs + slot * subs
            code = at[0] | at[1] << BITS | at[2] << 2 * BITS
            work[total] = code
            taken = slot < count
            hole = jnp.where(taken, hole, code)
            total = total + taken.astype(jnp.int32)
    for k in range(GROUP - 1):
        work[total + k] = hole
    return total


def group_of(got, work, ids, g, highs, lanes):
    codes = [work[g * GROUP + k] for k in range(GROUP)]
    mask = (1 << BITS) - 1
    v = [got[pl.ds((c >> BITS) & mask, 1), :].astype(jnp.int32) for c in codes]
    v = jnp.concatenate(v, axis=1)
    row = v // lanes
    high = jnp.where(v < 0, -1, row % highs)
    low = v % lanes + lanes * (row // highs)
    many = GROUP * lanes
    here = lax.broadcasted_iota(jnp.int32, (highs, many), 0) == high
    lows = jnp.broadcast_to(low.astype(jnp.float32), (16, many)).astype(jnp.bfloat16)
    one, zero = jnp.bfloat16(1.0), jnp.bfloat16(0.0)
    tiles = []
    for t in range(2 * lanes // 16):
        own = jnp.concatenate([ids[t * 16 : t * 16 + 16, :]] * GROUP, axis=1)
        tiles.append(jnp.where(own == lows, one, zero))
    return codes, here, jnp.concatenate(tiles, axis=0)


def cell_kernel(got, diffused, sums_out, back, acc, table, ids, work, *, slabs, subs):
    lanes = got.shape[1]
    channels = 2 * subs
    highs = diffused.shape[1] // 2
    wide = 2 * lanes
    mask = (1 << BITS) - 1
    total = list_blocks(got, work, slabs, subs)
    steps = (total + GROUP - 1) // GROUP
    acc[...] = jnp.zeros(acc.shape, jnp.float32)
    ids[...] = lax.broadcasted_iota(jnp.int32, ids.shape, 0).astype(jnp.float32).astype(jnp.bfloat16)

    def add(g, unused):
        codes, here, onehot = group_of(got, work, ids, g, highs, lanes)
        own = [got[pl.ds(pl.multiple_of(c & mask, 8), channels), :] for c in codes]
        high, low = halves(jnp.concatenate(own, axis=1))
        values = jnp.concatenate([high.astype(jnp.float32), low.astype(jnp.float32)], axis=0)
        spread = jnp.where(here[None], values[:, None, :], 0.0).astype(jnp.bfloat16)
        spread = spread.reshape(2 * channels * highs, GROUP * lanes)
        acc[...] += lax.dot_general(
            spread, onehot, (((1,), (1,)), ((), ())), preferred_element_type=jnp.float32
        )
        return unused

    lax.fori_loop(0, steps, add, 0)
    half = channels * highs
    sums = (acc[0:half, :] + acc[half : 2 * half, :]).reshape(channels, highs, wide)
    sums = jnp.concatenate([sums[:, :, :lanes], sums[:, :, lanes:]], axis=1)
    sums_out[...] = sums
    new = (diffused[...] + sums[:subs]) / (1.0 + sums[subs:])
    by_low = jnp.concatenate([new[:, :highs], new[:, highs:]], axis=2).reshape(subs * highs, wide)
    table[...] = jnp.concatenate(halves(by_low), axis=0)

    def read(g, unused):
        codes, here, onehot = group_of(got, work, ids, g, highs, lanes)
        rows = jnp.dot(table[...], onehot, preferred_element_type=jnp.float32)
        rows = (rows[: subs * highs] + rows[subs * highs :]).reshape(subs, highs, GROUP * lanes)
        found = jnp.sum(jnp.where(here[None], rows, 0.0), axis=1)
        for k, c in enumerate(codes):
            back[pl.ds(c >> 2 * BITS, subs), :] = found[:, k * lanes : (k + 1) * lanes]
        return unused

    lax.fori_loop(0, steps, read, 0)


def small(mebibytes):
    return pltpu.CompilerParams(vmem_limit_bytes=mebibytes << 20)


def vmem():
    return pl.BlockSpec(memory_space=pltpu.VMEM)


def smem():
    return pl.BlockSpec(memory_space=pltpu.SMEM)


def shards(field, diffusion, secrete, uptake, cell_voxel, block_dest):
    subs, lanes = field.shape[0], field.shape[3]
    lines = field.shape[1] * field.shape[2]
    blocks = block_dest.shape[0]
    cells = secrete.shape[1] // blocks
    slabs = lax.axis_size("gz")
    base, rows = rows_of(2 * subs)
    f32 = functools.partial(jax.ShapeDtypeStruct, dtype=jnp.float32)
    dest = block_dest.reshape(blocks)
    sent = pl.pallas_call(
        functools.partial(pack_kernel, subs=subs),
        out_shape=f32((slabs, rows, cells)),
        in_specs=[pl.BlockSpec(memory_space=pltpu.HBM)] * 4,
        out_specs=vmem(),
        scratch_shapes=[
            pltpu.SMEM((blocks,), jnp.int32),
            pltpu.VMEM((subs, blocks * cells), jnp.float32),
            pltpu.VMEM((subs, blocks * cells), jnp.float32),
            pltpu.VMEM((blocks, cells), jnp.int32),
            pltpu.SMEM((slabs,), jnp.int32),
            pltpu.SemaphoreType.DMA((4,)),
        ],
        name="pack",
    )(dest, secrete, uptake, cell_voxel.reshape(blocks, cells))
    got = lax.all_to_all(sent, "gz", split_axis=0, concat_axis=0, tiled=True)
    diffused = diffuse(field, diffusion).reshape(subs, lines, lanes)
    sums, back = pl.pallas_call(
        functools.partial(cell_kernel, slabs=slabs, subs=subs),
        out_shape=(f32((2 * subs, lines, lanes)), f32((slabs * CAP * subs, cells))),
        in_specs=[vmem(), vmem()],
        out_specs=(vmem(), vmem()),
        scratch_shapes=[
            pltpu.VMEM((4 * subs * lines // 2, 2 * lanes), jnp.float32),
            pltpu.VMEM((2 * subs * lines // 2, 2 * lanes), jnp.bfloat16),
            pltpu.VMEM((2 * lanes, lanes), jnp.bfloat16),
            pltpu.SMEM((slabs * CAP + GROUP,), jnp.int32),
        ],
        compiler_params=small(8),
        name="cells",
    )(got.reshape(slabs * rows, cells), diffused)
    back = back.reshape(slabs, CAP * subs, cells)
    came = lax.all_to_all(back, "gz", split_axis=0, concat_axis=0, tiled=True)
    cell_conc = pl.pallas_call(
        functools.partial(place_kernel, blocks=blocks, cells=cells, subs=subs),
        out_shape=f32((subs, blocks * cells)),
        in_specs=[smem(), vmem()],
        out_specs=vmem(),
        scratch_shapes=[pltpu.SMEM((slabs,), jnp.int32)],
        compiler_params=small(4),
        name="place",
    )(dest, came)
    new_field = (diffused + sums[:subs]) / (1.0 + sums[subs:])
    return (new_field.reshape(field.shape), cell_conc)


def solution(mesh):
    in_specs = (
        P("sa", ("grp", "gz"), "gy", None),
        P("sa"),
        P("sa", ("grp", "gz", "gy")),
        P("sa", ("grp", "gz", "gy")),
        P(("grp", "gz", "gy")),
        P(("grp", "gz", "gy"), None),
    )
    out_specs = (P("sa", ("grp", "gz"), "gy", None), P("sa", ("grp", "gz", "gy")))
    return jax.shard_map(shards, mesh=mesh, in_specs=in_specs, out_specs=out_specs, check_vma=False)
```

```python
import functools

import jax
import jax.numpy as jnp
from jax import lax
from jax.experimental import pallas as pl
from jax.experimental.pallas import tpu as pltpu
from jax.sharding import PartitionSpec as P

CAP = 6


def extended(x, sides, width):
    edges = {}
    for axis, dim in sides:
        size, length = (lax.axis_size(axis), x.shape[dim])
        up = [(i, (i + 1) % size) for i in range(size - 1)]
        last = lax.slice_in_dim(x, length - width, length, axis=dim)
        leading = lax.slice_in_dim(x, 0, width, axis=dim)
        edges[dim] = (
            lax.ppermute(last, axis, up),
            lax.ppermute(leading, axis, [(b, a) for a, b in up]),
        )
    done = []
    for _, dim in sides:
        low, high = edges[dim]
        around = [(width, width) if d in done else (0, 0) for d in range(x.ndim)]
        x = jnp.concatenate([jnp.pad(low, around), x, jnp.pad(high, around)], axis=dim)
        done.append(dim)
    return x


def neighbours(padded):
    beside_all = padded[:, 2:, 1:-1, 1:-1] + padded[:, :-2, 1:-1, 1:-1]
    beside_all = beside_all + padded[:, 1:-1, 2:, 1:-1] + padded[:, 1:-1, :-2, 1:-1]
    return beside_all + padded[:, 1:-1, 1:-1, 2:] + padded[:, 1:-1, 1:-1, :-2]


def diffuse(field, diffusion):
    padded = extended(field, (("gz", 1), ("gy", 2)), 1)
    padded = jnp.pad(padded, ((0, 0), (0, 0), (0, 0), (1, 1)))
    return field + diffusion[:, None, None, None] * (neighbours(padded) - 6.0 * field)


def rows_of(channels):
    return CAP * channels, -(-(CAP * channels + CAP) // 8) * 8


def pack_kernel(
    dest_in, secrete_in, uptake_in, voxel_in, out, dest, secrete, uptake, voxel, used, sems, *, subs
):
    pairs = ((dest_in, dest), (secrete_in, secrete), (uptake_in, uptake), (voxel_in, voxel))
    copies = [pltpu.make_async_copy(a, b, sems.at[i]) for i, (a, b) in enumerate(pairs)]
    for copy in copies:
        copy.start()
    slabs, _, cells = out.shape
    base, rows = rows_of(2 * subs)
    out[:, pl.ds(base, rows - base), :] = jnp.full((slabs, rows - base, cells), -1.0, jnp.float32)
    for i in range(slabs):
        used[i] = 0
    for copy in copies:
        copy.wait()
    for b in range(dest.shape[0]):
        to = dest[b]
        slot = used[to]
        used[to] = slot + 1
        at = slice(b * cells, (b + 1) * cells)
        out[to, pl.ds(slot * 2 * subs, subs), :] = secrete[:, at]
        out[to, pl.ds(slot * 2 * subs + subs, subs), :] = uptake[:, at]
        out[to, pl.ds(base + slot, 1), :] = voxel[b : b + 1, :].astype(jnp.float32)
    for i in range(slabs):
        out[i, base + CAP : base + CAP + 1, :] = jnp.full((1, cells), used[i]).astype(jnp.float32)


def place_kernel(dest, came, out, used, *, blocks, cells, subs):
    for i in range(came.shape[0]):
        used[i] = 0
    for b in range(blocks):
        to = dest[b]
        slot = used[to]
        used[to] = slot + 1
        out[:, b * cells : (b + 1) * cells] = came[to, pl.ds(slot * subs, subs), :]


def halves(x):
    high = x.astype(jnp.bfloat16)
    return high, (x - high.astype(jnp.float32)).astype(jnp.bfloat16)


GROUP, PART = 32, 2
BITS = 10


def list_blocks(got, work, slabs, subs):
    base, rows = rows_of(2 * subs)
    counts = jnp.concatenate([got[i * rows + base + CAP : i * rows + base + CAP + 1, :] for i in range(slabs)], axis=0)
    lane = lax.broadcasted_iota(jnp.int32, (8, counts.shape[1]), 1)
    digit = lax.broadcasted_iota(jnp.int32, (8, counts.shape[1]), 0)
    scale = jnp.where(lane == 0, 1 << (3 * digit), 0).astype(jnp.float32)
    words = [jnp.sum(counts[8 * w : 8 * w + 8] * scale).astype(jnp.int32) for w in range(slabs // 8)]
    total, hole = jnp.int32(0), jnp.int32(0)
    for i in range(slabs):
        count = (words[i // 8] >> (3 * (i % 8))) & 7
        for slot in range(CAP):
            at = i * rows + slot * 2 * subs, i * rows + base + slot, i * CAP * subs + slot * subs
            code = at[0] | at[1] << BITS | at[2] << 2 * BITS
            work[total] = code
            taken = slot < count
            hole = jnp.where(taken, hole, code)
            total = total + taken.astype(jnp.int32)
    for k in range(GROUP - 1):
        work[total + k] = hole
    return total


def part_of(got, codes, ids, highs, lanes):
    mask = (1 << BITS) - 1
    v = [got[pl.ds((c >> BITS) & mask, 1), :].astype(jnp.int32) for c in codes]
    v = jnp.concatenate(v, axis=1)
    row = v // lanes
    high = jnp.where(v < 0, -1, row % highs)
    low = v % lanes + lanes * (row // highs)
    many = len(codes) * lanes
    here = lax.broadcasted_iota(jnp.int32, (highs, many), 0) == high
    lows = jnp.broadcast_to(low.astype(jnp.float32), (16, many)).astype(jnp.bfloat16)
    one, zero = jnp.bfloat16(1.0), jnp.bfloat16(0.0)
    tiles = []
    for t in range(2 * lanes // 16):
        own = jnp.concatenate([ids[t * 16 : t * 16 + 16, :]] * len(codes), axis=1)
        tiles.append(jnp.where(own == lows, one, zero))
    return here, jnp.concatenate(tiles, axis=0)


def cell_kernel(got, diffused, sums_out, back, acc, table, ids, work, *, slabs, subs):
    lanes = got.shape[1]
    channels = 2 * subs
    highs = diffused.shape[1] // 2
    wide = 2 * lanes
    mask = (1 << BITS) - 1
    total = list_blocks(got, work, slabs, subs)
    steps = (total + GROUP - 1) // GROUP
    acc[...] = jnp.zeros(acc.shape, jnp.float32)
    ids[...] = lax.broadcasted_iota(jnp.int32, ids.shape, 0).astype(jnp.float32).astype(jnp.bfloat16)

    def parts(g):
        return [[work[g * GROUP + p + k] for k in range(PART)] for p in range(0, GROUP, PART)]

    def add(g, unused):
        partial = []
        for codes in parts(g):
            here, onehot = part_of(got, codes, ids, highs, lanes)
            own = [got[pl.ds(pl.multiple_of(c & mask, 8), channels), :] for c in codes]
            high, low = halves(jnp.concatenate(own, axis=1))
            values = jnp.concatenate([high.astype(jnp.float32), low.astype(jnp.float32)], axis=0)
            spread = jnp.where(here[None], values[:, None, :], 0.0).astype(jnp.bfloat16)
            spread = spread.reshape(2 * channels * highs, PART * lanes)
            partial.append(
                lax.dot_general(
                    spread, onehot, (((1,), (1,)), ((), ())), preferred_element_type=jnp.float32
                )
            )
        acc[...] += sum(partial[1:], partial[0])
        return unused

    lax.fori_loop(0, steps, add, 0)
    half = channels * highs
    sums = (acc[0:half, :] + acc[half : 2 * half, :]).reshape(channels, highs, wide)
    sums = jnp.concatenate([sums[:, :, :lanes], sums[:, :, lanes:]], axis=1)
    sums_out[...] = sums
    new = (diffused[...] + sums[:subs]) / (1.0 + sums[subs:])
    by_low = jnp.concatenate([new[:, :highs], new[:, highs:]], axis=2).reshape(subs * highs, wide)
    table[...] = jnp.concatenate(halves(by_low), axis=0)

    def read(g, unused):
        for codes in parts(g):
            here, onehot = part_of(got, codes, ids, highs, lanes)
            rows = jnp.dot(table[...], onehot, preferred_element_type=jnp.float32)
            rows = (rows[: subs * highs] + rows[subs * highs :]).reshape(subs, highs, PART * lanes)
            found = jnp.sum(jnp.where(here[None], rows, 0.0), axis=1)
            for k, c in enumerate(codes):
                back[pl.ds(c >> 2 * BITS, subs), :] = found[:, k * lanes : (k + 1) * lanes]
        return unused

    lax.fori_loop(0, steps, read, 0)


def small(mebibytes):
    return pltpu.CompilerParams(vmem_limit_bytes=mebibytes << 20)


def vmem():
    return pl.BlockSpec(memory_space=pltpu.VMEM)


def smem():
    return pl.BlockSpec(memory_space=pltpu.SMEM)


def call_cells(got, diffused, slabs, subs):
    lines, lanes = diffused.shape[1:]
    f32 = functools.partial(jax.ShapeDtypeStruct, dtype=jnp.float32)
    return pl.pallas_call(
        functools.partial(cell_kernel, slabs=slabs, subs=subs),
        out_shape=(f32((2 * subs, lines, lanes)), f32((slabs * CAP * subs, lanes))),
        in_specs=[vmem(), vmem()],
        out_specs=(vmem(), vmem()),
        scratch_shapes=[
            pltpu.VMEM((4 * subs * lines // 2, 2 * lanes), jnp.float32),
            pltpu.VMEM((2 * subs * lines // 2, 2 * lanes), jnp.bfloat16),
            pltpu.VMEM((2 * lanes, lanes), jnp.bfloat16),
            pltpu.SMEM((slabs * CAP + GROUP,), jnp.int32),
        ],
        compiler_params=small(8),
        name="cells",
    )(got, diffused)


def shards(field, diffusion, secrete, uptake, cell_voxel, block_dest):
    subs, lanes = field.shape[0], field.shape[3]
    lines = field.shape[1] * field.shape[2]
    blocks = block_dest.shape[0]
    cells = secrete.shape[1] // blocks
    slabs = lax.axis_size("gz")
    base, rows = rows_of(2 * subs)
    f32 = functools.partial(jax.ShapeDtypeStruct, dtype=jnp.float32)
    dest = block_dest.reshape(blocks)
    sent = pl.pallas_call(
        functools.partial(pack_kernel, subs=subs),
        out_shape=f32((slabs, rows, cells)),
        in_specs=[pl.BlockSpec(memory_space=pltpu.HBM)] * 4,
        out_specs=vmem(),
        scratch_shapes=[
            pltpu.SMEM((blocks,), jnp.int32),
            pltpu.VMEM((subs, blocks * cells), jnp.float32),
            pltpu.VMEM((subs, blocks * cells), jnp.float32),
            pltpu.VMEM((blocks, cells), jnp.int32),
            pltpu.SMEM((slabs,), jnp.int32),
            pltpu.SemaphoreType.DMA((4,)),
        ],
        name="pack",
    )(dest, secrete, uptake, cell_voxel.reshape(blocks, cells))
    got = lax.all_to_all(sent, "gz", split_axis=0, concat_axis=0, tiled=True)
    diffused = diffuse(field, diffusion).reshape(subs, lines, lanes)
    sums, back = call_cells(got.reshape(slabs * rows, cells), diffused, slabs, subs)
    back = back.reshape(slabs, CAP * subs, cells)
    came = lax.all_to_all(back, "gz", split_axis=0, concat_axis=0, tiled=True)
    cell_conc = pl.pallas_call(
        functools.partial(place_kernel, blocks=blocks, cells=cells, subs=subs),
        out_shape=f32((subs, blocks * cells)),
        in_specs=[smem(), vmem()],
        out_specs=vmem(),
        scratch_shapes=[pltpu.SMEM((slabs,), jnp.int32)],
        compiler_params=small(4),
        name="place",
    )(dest, came)
    new_field = (diffused + sums[:subs]) / (1.0 + sums[subs:])
    return (new_field.reshape(field.shape), cell_conc)


def solution(mesh):
    in_specs = (
        P("sa", ("grp", "gz"), "gy", None),
        P("sa"),
        P("sa", ("grp", "gz", "gy")),
        P("sa", ("grp", "gz", "gy")),
        P(("grp", "gz", "gy")),
        P(("grp", "gz", "gy"), None),
    )
    out_specs = (P("sa", ("grp", "gz"), "gy", None), P("sa", ("grp", "gz", "gy")))
    return jax.shard_map(shards, mesh=mesh, in_specs=in_specs, out_specs=out_specs, check_vma=False)
```

```python
import functools

import jax
import jax.numpy as jnp
from jax import lax
from jax.experimental import pallas as pl
from jax.experimental.pallas import tpu as pltpu
from jax.sharding import PartitionSpec as P

CAP = 6


def extended(x, sides, width):
    edges = {}
    for axis, dim in sides:
        size, length = (lax.axis_size(axis), x.shape[dim])
        up = [(i, (i + 1) % size) for i in range(size - 1)]
        last = lax.slice_in_dim(x, length - width, length, axis=dim)
        leading = lax.slice_in_dim(x, 0, width, axis=dim)
        edges[dim] = (
            lax.ppermute(last, axis, up),
            lax.ppermute(leading, axis, [(b, a) for a, b in up]),
        )
    done = []
    for _, dim in sides:
        low, high = edges[dim]
        around = [(width, width) if d in done else (0, 0) for d in range(x.ndim)]
        x = jnp.concatenate([jnp.pad(low, around), x, jnp.pad(high, around)], axis=dim)
        done.append(dim)
    return x


def neighbours(padded):
    beside_all = padded[:, 2:, 1:-1, 1:-1] + padded[:, :-2, 1:-1, 1:-1]
    beside_all = beside_all + padded[:, 1:-1, 2:, 1:-1] + padded[:, 1:-1, :-2, 1:-1]
    return beside_all + padded[:, 1:-1, 1:-1, 2:] + padded[:, 1:-1, 1:-1, :-2]


def diffuse(field, diffusion):
    padded = extended(field, (("gz", 1), ("gy", 2)), 1)
    padded = jnp.pad(padded, ((0, 0), (0, 0), (0, 0), (1, 1)))
    return field + diffusion[:, None, None, None] * (neighbours(padded) - 6.0 * field)


def rows_of(channels):
    return CAP * channels, CAP * channels + CAP


def pack_kernel(
    dest_in, secrete_in, uptake_in, voxel_in, out, dest, secrete, uptake, voxel, used, sems, *, slabs, subs
):
    pairs = ((dest_in, dest), (secrete_in, secrete), (uptake_in, uptake), (voxel_in, voxel))
    copies = [pltpu.make_async_copy(a, b, sems.at[i]) for i, (a, b) in enumerate(pairs)]
    for copy in copies:
        copy.start()
    cells = out.shape[1]
    base, rows = rows_of(2 * subs)
    for i in range(slabs):
        out[i * rows + base : (i + 1) * rows, :] = jnp.full((rows - base, cells), -1.0, jnp.float32)
        used[i] = 0
    for copy in copies:
        copy.wait()
    for b in range(dest.shape[0]):
        to = dest[b]
        slot = used[to]
        used[to] = slot + 1
        at = slice(b * cells, (b + 1) * cells)
        first = to * rows + slot * 2 * subs
        out[pl.ds(first, subs), :] = secrete[:, at]
        out[pl.ds(first + subs, subs), :] = uptake[:, at]
        out[pl.ds(to * rows + base + slot, 1), :] = voxel[b : b + 1, :].astype(jnp.float32)


def place_kernel(dest, came, out, used, *, blocks, cells, subs):
    for i in range(came.shape[0]):
        used[i] = 0
    for b in range(blocks):
        to = dest[b]
        slot = used[to]
        used[to] = slot + 1
        out[:, b * cells : (b + 1) * cells] = came[to, pl.ds(slot * subs, subs), :]


def halves(x):
    high = x.astype(jnp.bfloat16)
    return high, (x - high.astype(jnp.float32)).astype(jnp.bfloat16)


GROUP, PART = 48, 2
BITS = 10


def list_blocks(got, work, high_of, low_of, slabs, subs, highs):
    base, rows = rows_of(2 * subs)
    lanes = got.shape[1]
    lane_bits, high_bits = lanes.bit_length() - 1, highs.bit_length() - 1
    lane = lax.broadcasted_iota(jnp.int32, (CAP, lanes), 1)
    words, total, hole = [], jnp.int32(0), jnp.int32(0)
    for w in range(slabs // 8):
        marks = jnp.zeros((CAP, lanes), jnp.float32)
        for k in range(8):
            i = w * 8 + k
            v = got[i * rows + base : (i + 1) * rows, :].astype(jnp.int32)
            row = v >> lane_bits
            here = v >= 0
            high = jnp.where(here, row & (highs - 1), -1)
            low = (v & (lanes - 1)) | ((row >> high_bits) << lane_bits)
            high_of[i * CAP : (i + 1) * CAP, :] = high.astype(jnp.float32)
            low_of[i * CAP : (i + 1) * CAP, :] = low.astype(jnp.float32)
            marks = marks + jnp.where(here & (lane == 0), float(8**k), 0.0)
        words.append(jnp.sum(marks).astype(jnp.int32))
    for i in range(slabs):
        count = (words[i // 8] >> (3 * (i % 8))) & 7
        for slot in range(CAP):
            at = i * rows + slot * 2 * subs, i * CAP + slot, (i * CAP + slot) * subs
            code = at[0] | at[1] << BITS | at[2] << 2 * BITS
            work[total + slot] = code
        hole = jnp.where(count < CAP, code, hole)
        total = total + count
    for k in range(GROUP - 1):
        work[total + k] = hole
    return total


def spread_row(ref, row):
    own = ref[pl.ds(row, 8, stride=0), :]
    return jnp.concatenate([own, own], axis=0).astype(jnp.bfloat16)


def onehots_of(ids, lows, wide):
    tiles = []
    for t in range(0, wide, 16):
        own = ids[t : t + 16, :].astype(jnp.bfloat16)
        row = [jnp.where(own == low, jnp.bfloat16(1.0), jnp.bfloat16(0.0)) for low in lows]
        tiles.append(jnp.concatenate(row, axis=1))
    return jnp.concatenate(tiles, axis=0)


def cell_kernel(
    got, diffused, sums_out, back, acc, table, ids, high_of, low_of, split, found, work, *, slabs, subs
):
    lanes = got.shape[1]
    channels = 2 * subs
    highs = diffused.shape[1] // 2
    wide = 2 * lanes
    mask = (1 << BITS) - 1
    total = list_blocks(got, work, high_of, low_of, slabs, subs, highs)
    steps = (total + GROUP - 1) // GROUP
    acc[...] = jnp.zeros(acc.shape, jnp.float32)
    ids[...] = lax.broadcasted_iota(jnp.int32, ids.shape, 0).astype(jnp.float32)

    def add(g, unused):
        partial = []
        first = ids[0:highs, :].astype(jnp.bfloat16)
        for p in range(0, GROUP, PART):
            spreads, lows = [], []
            for k in range(p, p + PART):
                code = work[g * GROUP + k]
                slot = (code >> BITS) & mask
                high, low = halves(got[pl.ds(code & mask, channels), :])
                at = k * 2 * channels
                split[at : at + channels, :] = high.astype(jnp.float32)
                split[at + channels : at + 2 * channels, :] = low.astype(jnp.float32)
                here = first == spread_row(high_of, slot)
                own = [jnp.where(here, spread_row(split, at + r), jnp.bfloat16(0.0)) for r in range(2 * channels)]
                spreads.append(jnp.concatenate(own, axis=0))
                lows.append(spread_row(low_of, slot))
            partial.append(
                lax.dot_general(
                    jnp.concatenate(spreads, axis=1),
                    onehots_of(ids, lows, wide),
                    (((1,), (1,)), ((), ())),
                    preferred_element_type=jnp.float32,
                )
            )
        acc[...] += sum(partial[1:], partial[0])
        return unused

    lax.fori_loop(0, steps, add, 0)
    half = channels * highs
    sums = (acc[0:half, :] + acc[half : 2 * half, :]).reshape(channels, highs, wide)
    sums = jnp.concatenate([sums[:, :, :lanes], sums[:, :, lanes:]], axis=1)
    sums_out[...] = sums
    new = (diffused[...] + sums[:subs]) / (1.0 + sums[subs:])
    by_low = jnp.concatenate([new[:, :highs], new[:, highs:]], axis=2).reshape(subs * highs, wide)
    table[...] = jnp.concatenate([h.astype(jnp.float32) for h in halves(by_low)], axis=0)

    sub = lax.broadcasted_iota(jnp.int32, (8, lanes), 0)
    subf = sub.astype(jnp.float32)

    def read(g, unused):
        values = table[...].astype(jnp.bfloat16)
        for p in range(0, GROUP, PART):
            codes = [work[g * GROUP + k] for k in range(p, p + PART)]
            slots = [(code >> BITS) & mask for code in codes]
            onehot = onehots_of(ids, [spread_row(low_of, slot) for slot in slots], wide)
            rows = jnp.dot(values, onehot, preferred_element_type=jnp.float32)
            rows = rows[: subs * highs] + rows[subs * highs :]
            for k in range(PART):
                own = rows[:, k * lanes : (k + 1) * lanes]
                high = high_of[pl.ds(slots[k], 8, stride=0), :]
                at = 8 * (p + k)
                found[at : at + 8, :] = found_rows(own, subf == high, subf + 8.0 == high, sub, subs, highs)
                back[pl.ds(codes[k] >> 2 * BITS, subs), :] = found[pl.ds(at + 1, subs, stride=2), :]
        return unused

    lax.fori_loop(0, steps, read, 0)


def found_rows(own, first, second, sub, subs, highs):
    assert subs == 4 and highs == 16
    fours = []
    for s in range(subs):
        a = own[s * highs : s * highs + 8, :]
        b = own[s * highs + 8 : s * highs + 16, :]
        x = jnp.where(first, a, jnp.where(second, b, 0.0))
        fours.append(x + pltpu.roll(x, 4, 0))
    upper = jnp.where(sub < 4, fours[1], fours[3])
    lower = jnp.where(sub < 4, fours[0], fours[2])
    upper = upper + pltpu.roll(upper, 2, 0)
    lower = lower + pltpu.roll(lower, 2, 0)
    both = jnp.where((sub & 2) == 2, upper, pltpu.roll(lower, 6, 0))
    return both + pltpu.roll(both, 1, 0)


def small(mebibytes):
    return pltpu.CompilerParams(vmem_limit_bytes=mebibytes << 20)


def vmem():
    return pl.BlockSpec(memory_space=pltpu.VMEM)


def smem():
    return pl.BlockSpec(memory_space=pltpu.SMEM)


def call_cells(got, diffused, slabs, subs):
    lines, lanes = diffused.shape[1:]
    f32 = functools.partial(jax.ShapeDtypeStruct, dtype=jnp.float32)
    return pl.pallas_call(
        functools.partial(cell_kernel, slabs=slabs, subs=subs),
        out_shape=(f32((2 * subs, lines, lanes)), f32((slabs * CAP * subs, lanes))),
        in_specs=[vmem(), vmem()],
        out_specs=(vmem(), vmem()),
        scratch_shapes=[
            pltpu.VMEM((4 * subs * lines // 2, 2 * lanes), jnp.float32),
            pltpu.VMEM((2 * subs * lines // 2, 2 * lanes), jnp.float32),
            pltpu.VMEM((2 * lanes, lanes), jnp.float32),
            pltpu.VMEM((slabs * CAP, lanes), jnp.float32),
            pltpu.VMEM((slabs * CAP, lanes), jnp.float32),
            pltpu.VMEM((GROUP * 4 * subs, lanes), jnp.float32),
            pltpu.VMEM((GROUP * 8, lanes), jnp.float32),
            pltpu.SMEM((slabs * CAP + GROUP + CAP,), jnp.int32),
        ],
        compiler_params=small(8),
        name="cells",
    )(got, diffused)


def shards(field, diffusion, secrete, uptake, cell_voxel, block_dest):
    subs, lanes = field.shape[0], field.shape[3]
    lines = field.shape[1] * field.shape[2]
    blocks = block_dest.shape[0]
    cells = secrete.shape[1] // blocks
    slabs = lax.axis_size("gz")
    base, rows = rows_of(2 * subs)
    f32 = functools.partial(jax.ShapeDtypeStruct, dtype=jnp.float32)
    dest = block_dest.reshape(blocks)
    sent = pl.pallas_call(
        functools.partial(pack_kernel, slabs=slabs, subs=subs),
        out_shape=f32((slabs * rows, cells)),
        in_specs=[pl.BlockSpec(memory_space=pltpu.HBM)] * 4,
        out_specs=vmem(),
        scratch_shapes=[
            pltpu.SMEM((blocks,), jnp.int32),
            pltpu.VMEM((subs, blocks * cells), jnp.float32),
            pltpu.VMEM((subs, blocks * cells), jnp.float32),
            pltpu.VMEM((blocks, cells), jnp.int32),
            pltpu.SMEM((slabs,), jnp.int32),
            pltpu.SemaphoreType.DMA((4,)),
        ],
        name="pack",
    )(dest, secrete, uptake, cell_voxel.reshape(blocks, cells))
    sent = sent.reshape(slabs, rows // 2, 2, cells)
    got = lax.all_to_all(sent, "gz", split_axis=0, concat_axis=0, tiled=True)
    diffused = diffuse(field, diffusion).reshape(subs, lines, lanes)
    sums, back = call_cells(got.reshape(slabs * rows, cells), diffused, slabs, subs)
    back = back.reshape(slabs, CAP * subs, cells)
    came = lax.all_to_all(back, "gz", split_axis=0, concat_axis=0, tiled=True)
    cell_conc = pl.pallas_call(
        functools.partial(place_kernel, blocks=blocks, cells=cells, subs=subs),
        out_shape=f32((subs, blocks * cells)),
        in_specs=[smem(), vmem()],
        out_specs=vmem(),
        scratch_shapes=[pltpu.SMEM((slabs,), jnp.int32)],
        compiler_params=small(4),
        name="place",
    )(dest, came)
    new_field = (diffused + sums[:subs]) / (1.0 + sums[subs:])
    return (new_field.reshape(field.shape), cell_conc)


def solution(mesh):
    in_specs = (
        P("sa", ("grp", "gz"), "gy", None),
        P("sa"),
        P("sa", ("grp", "gz", "gy")),
        P("sa", ("grp", "gz", "gy")),
        P(("grp", "gz", "gy")),
        P(("grp", "gz", "gy"), None),
    )
    out_specs = (P("sa", ("grp", "gz"), "gy", None), P("sa", ("grp", "gz", "gy")))
    return jax.shard_map(shards, mesh=mesh, in_specs=in_specs, out_specs=out_specs, check_vma=False)
```

```python
import functools

import jax
import jax.numpy as jnp
from jax import lax
from jax.experimental import pallas as pl
from jax.experimental.pallas import tpu as pltpu
from jax.sharding import PartitionSpec as P

CAP = 6


def extended(x, sides, width):
    edges = {}
    for axis, dim in sides:
        size, length = (lax.axis_size(axis), x.shape[dim])
        up = [(i, (i + 1) % size) for i in range(size - 1)]
        last = lax.slice_in_dim(x, length - width, length, axis=dim)
        leading = lax.slice_in_dim(x, 0, width, axis=dim)
        edges[dim] = (
            lax.ppermute(last, axis, up),
            lax.ppermute(leading, axis, [(b, a) for a, b in up]),
        )
    done = []
    for _, dim in sides:
        low, high = edges[dim]
        around = [(width, width) if d in done else (0, 0) for d in range(x.ndim)]
        x = jnp.concatenate([jnp.pad(low, around), x, jnp.pad(high, around)], axis=dim)
        done.append(dim)
    return x


def neighbours(padded):
    beside_all = padded[:, 2:, 1:-1, 1:-1] + padded[:, :-2, 1:-1, 1:-1]
    beside_all = beside_all + padded[:, 1:-1, 2:, 1:-1] + padded[:, 1:-1, :-2, 1:-1]
    return beside_all + padded[:, 1:-1, 1:-1, 2:] + padded[:, 1:-1, 1:-1, :-2]


def diffuse(field, diffusion):
    padded = extended(field, (("gz", 1), ("gy", 2)), 1)
    padded = jnp.pad(padded, ((0, 0), (0, 0), (0, 0), (1, 1)))
    return field + diffusion[:, None, None, None] * (neighbours(padded) - 6.0 * field)


def rows_of(channels):
    return CAP * channels, CAP * channels + CAP


def pack_kernel(
    dest_in, secrete_in, uptake_in, voxel_in, out, dest, secrete, uptake, voxel, used, sems, *, slabs, subs
):
    pairs = ((dest_in, dest), (secrete_in, secrete), (uptake_in, uptake), (voxel_in, voxel))
    copies = [pltpu.make_async_copy(a, b, sems.at[i]) for i, (a, b) in enumerate(pairs)]
    for copy in copies:
        copy.start()
    cells = out.shape[1]
    base, rows = rows_of(2 * subs)
    for i in range(slabs):
        out[i * rows + base : (i + 1) * rows, :] = jnp.full((rows - base, cells), -1.0, jnp.float32)
        used[i] = 0
    for copy in copies:
        copy.wait()
    for b in range(dest.shape[0]):
        to = dest[b]
        slot = used[to]
        used[to] = slot + 1
        at = slice(b * cells, (b + 1) * cells)
        first = to * rows + slot * 2 * subs
        out[pl.ds(first, subs), :] = secrete[:, at]
        out[pl.ds(first + subs, subs), :] = uptake[:, at]
        out[pl.ds(to * rows + base + slot, 1), :] = voxel[b : b + 1, :].astype(jnp.float32)


def place_kernel(first, came, new, out, new_field, used, *, blocks, cells, subs):
    new_field[...] = new[...]
    for i in range(0, came.shape[0] // subs, CAP):
        used[i] = i
    for b in range(blocks):
        slab = first[b]
        slot = used[slab]
        used[slab] = slot + 1
        out[:, b * cells : (b + 1) * cells] = came[pl.ds(slot * subs, subs), :]


def halves(x):
    high = x.astype(jnp.bfloat16)
    return high, (x - high.astype(jnp.float32)).astype(jnp.bfloat16)


SIZES, PART = (32, 40, 48, 96), 2
BITS = 10


def list_blocks(got, work, high_of, low_of, slabs, subs, highs):
    base, rows = rows_of(2 * subs)
    lanes = got.shape[1]
    lane_bits, high_bits = lanes.bit_length() - 1, highs.bit_length() - 1
    lane = lax.broadcasted_iota(jnp.int32, (CAP, lanes), 1)
    words, total, hole = [], jnp.int32(0), jnp.int32(0)
    for w in range(slabs // 8):
        marks = jnp.zeros((CAP, lanes), jnp.float32)
        for k in range(8):
            i = w * 8 + k
            v = got[i * rows + base : (i + 1) * rows, :].astype(jnp.int32)
            row = v >> lane_bits
            here = v >= 0
            high = jnp.where(here, row & (highs - 1), -1)
            low = (v & (lanes - 1)) | ((row >> high_bits) << lane_bits)
            high_of[i * CAP : (i + 1) * CAP, :] = high.astype(jnp.float32)
            low_of[i * CAP : (i + 1) * CAP, :] = low.astype(jnp.float32)
            marks = marks + jnp.where(here & (lane == 0), float(8**k), 0.0)
        words.append(jnp.sum(marks).astype(jnp.int32))
    for i in range(slabs):
        count = (words[i // 8] >> (3 * (i % 8))) & 7
        for slot in range(CAP):
            at = i * rows + slot * 2 * subs, i * CAP + slot, (i * CAP + slot) * subs
            code = at[0] | at[1] << BITS | at[2] << 2 * BITS
            work[total + slot] = code
        hole = jnp.where(count < CAP, code, hole)
        total = total + count
    for k in range(SIZES[-1] // 2):
        work[total + k] = hole
    return total


def spread_row(ref, row):
    own = ref[pl.ds(row, 8, stride=0), :]
    return jnp.concatenate([own, own], axis=0).astype(jnp.bfloat16)


def onehots_of(ids, lows, wide):
    tiles = []
    for t in range(0, wide, 16):
        own = ids[t : t + 16, :].astype(jnp.bfloat16)
        row = [jnp.where(own == low, jnp.bfloat16(1.0), jnp.bfloat16(0.0)) for low in lows]
        tiles.append(jnp.concatenate(row, axis=1))
    return jnp.concatenate(tiles, axis=0)


def cell_kernel(
    got, diffused, dest_in, new_out, back, dest_out, acc, table, ids, high_of, low_of, split, found, work, *, slabs, subs
):
    lanes = got.shape[1]
    channels = 2 * subs
    highs = diffused.shape[1] // 2
    wide = 2 * lanes
    mask = (1 << BITS) - 1
    total = list_blocks(got, work, high_of, low_of, slabs, subs, highs)
    ids[...] = lax.broadcasted_iota(jnp.int32, ids.shape, 0).astype(jnp.float32)

    def at_size(body):
        below = -1
        for size in SIZES:
            pl.when((total > below) & (total <= size))(functools.partial(body, size))
            below = size

    def add(size):
        partial = []
        first = ids[0:highs, :].astype(jnp.bfloat16)
        for p in range(0, size, PART):
            spreads, lows = [], []
            for k in range(p, p + PART):
                code = work[k]
                slot = (code >> BITS) & mask
                high, low = halves(got[pl.ds(code & mask, channels), :])
                at = k * 2 * channels
                split[at : at + channels, :] = high.astype(jnp.float32)
                split[at + channels : at + 2 * channels, :] = low.astype(jnp.float32)
                here = first == spread_row(high_of, slot)
                own = [jnp.where(here, spread_row(split, at + r), jnp.bfloat16(0.0)) for r in range(2 * channels)]
                spreads.append(jnp.concatenate(own, axis=0))
                lows.append(spread_row(low_of, slot))
            partial.append(
                lax.dot_general(
                    jnp.concatenate(spreads, axis=1),
                    onehots_of(ids, lows, wide),
                    (((1,), (1,)), ((), ())),
                    preferred_element_type=jnp.float32,
                )
            )
        acc[...] = sum(partial[1:], partial[0])

    at_size(add)
    half = channels * highs
    sums = (acc[0:half, :] + acc[half : 2 * half, :]).reshape(channels, highs, wide)
    sums = jnp.concatenate([sums[:, :, :lanes], sums[:, :, lanes:]], axis=1)
    new = (diffused[...] + sums[:subs]) / (1.0 + sums[subs:])
    new_out[...] = new
    dest_out[...] = dest_in[...]
    by_low = jnp.concatenate([new[:, :highs], new[:, highs:]], axis=2).reshape(subs * highs, wide)
    table[...] = jnp.concatenate([h.astype(jnp.float32) for h in halves(by_low)], axis=0)

    sub = lax.broadcasted_iota(jnp.int32, (8, lanes), 0)
    subf = sub.astype(jnp.float32)

    def read(size):
        values = table[...].astype(jnp.bfloat16)
        for p in range(0, size, PART):
            codes = [work[k] for k in range(p, p + PART)]
            slots = [(code >> BITS) & mask for code in codes]
            onehot = onehots_of(ids, [spread_row(low_of, slot) for slot in slots], wide)
            rows = jnp.dot(values, onehot, preferred_element_type=jnp.float32)
            rows = rows[: subs * highs] + rows[subs * highs :]
            for k in range(PART):
                own = rows[:, k * lanes : (k + 1) * lanes]
                high = high_of[pl.ds(slots[k], 8, stride=0), :]
                at = 8 * (p + k)
                found[at : at + 8, :] = found_rows(own, subf == high, subf + 8.0 == high, sub, subs, highs)
                back[pl.ds(codes[k] >> 2 * BITS, subs), :] = found[pl.ds(at + 1, subs, stride=2), :]

    at_size(read)


def found_rows(own, first, second, sub, subs, highs):
    assert subs == 4 and highs == 16
    fours = []
    for s in range(subs):
        a = own[s * highs : s * highs + 8, :]
        b = own[s * highs + 8 : s * highs + 16, :]
        x = jnp.where(first, a, jnp.where(second, b, 0.0))
        fours.append(x + pltpu.roll(x, 4, 0))
    upper = jnp.where(sub < 4, fours[1], fours[3])
    lower = jnp.where(sub < 4, fours[0], fours[2])
    upper = upper + pltpu.roll(upper, 2, 0)
    lower = lower + pltpu.roll(lower, 2, 0)
    both = jnp.where((sub & 2) == 2, upper, pltpu.roll(lower, 6, 0))
    return both + pltpu.roll(both, 1, 0)


def small(mebibytes):
    return pltpu.CompilerParams(vmem_limit_bytes=mebibytes << 20)


def vmem():
    return pl.BlockSpec(memory_space=pltpu.VMEM)


def smem():
    return pl.BlockSpec(memory_space=pltpu.SMEM)


def call_cells(got, diffused, dest, slabs, subs):
    lines, lanes = diffused.shape[1:]
    f32 = functools.partial(jax.ShapeDtypeStruct, dtype=jnp.float32)
    return pl.pallas_call(
        functools.partial(cell_kernel, slabs=slabs, subs=subs),
        out_shape=(f32((subs, lines, lanes)), f32((slabs * CAP * subs, lanes)), jax.ShapeDtypeStruct(dest.shape, dest.dtype)),
        in_specs=[vmem(), vmem(), vmem()],
        out_specs=(vmem(), vmem(), vmem()),
        scratch_shapes=[
            pltpu.VMEM((4 * subs * lines // 2, 2 * lanes), jnp.float32),
            pltpu.VMEM((2 * subs * lines // 2, 2 * lanes), jnp.float32),
            pltpu.VMEM((2 * lanes, lanes), jnp.float32),
            pltpu.VMEM((slabs * CAP, lanes), jnp.float32),
            pltpu.VMEM((slabs * CAP, lanes), jnp.float32),
            pltpu.VMEM((slabs * CAP * 4 * subs, lanes), jnp.float32),
            pltpu.VMEM((slabs * CAP * 8, lanes), jnp.float32),
            pltpu.SMEM((2 * slabs * CAP,), jnp.int32),
        ],
        compiler_params=small(8),
        name="cells",
    )(got, diffused, dest)


def shards(field, diffusion, secrete, uptake, cell_voxel, block_dest):
    subs, lanes = field.shape[0], field.shape[3]
    lines = field.shape[1] * field.shape[2]
    blocks = block_dest.shape[0]
    cells = secrete.shape[1] // blocks
    slabs = lax.axis_size("gz")
    base, rows = rows_of(2 * subs)
    f32 = functools.partial(jax.ShapeDtypeStruct, dtype=jnp.float32)
    dest = block_dest.reshape(blocks)
    sent = pl.pallas_call(
        functools.partial(pack_kernel, slabs=slabs, subs=subs),
        out_shape=f32((slabs * rows, cells)),
        in_specs=[pl.BlockSpec(memory_space=pltpu.HBM)] * 4,
        out_specs=vmem(),
        scratch_shapes=[
            pltpu.SMEM((blocks,), jnp.int32),
            pltpu.VMEM((subs, blocks * cells), jnp.float32),
            pltpu.VMEM((subs, blocks * cells), jnp.float32),
            pltpu.VMEM((blocks, cells), jnp.int32),
            pltpu.SMEM((slabs,), jnp.int32),
            pltpu.SemaphoreType.DMA((4,)),
        ],
        name="pack",
    )(dest, secrete, uptake, cell_voxel.reshape(blocks, cells))
    sent = sent.reshape(slabs, rows // 2, 2, cells)
    got = lax.all_to_all(sent, "gz", split_axis=0, concat_axis=0, tiled=True)
    diffused = diffuse(field, diffusion).reshape(subs, lines, lanes)
    new, back, first = call_cells(got.reshape(slabs * rows, cells), diffused, block_dest.reshape(1, blocks) * CAP, slabs, subs)
    back = back.reshape(slabs, CAP * subs, cells)
    came = lax.all_to_all(back, "gz", split_axis=0, concat_axis=0, tiled=True)
    cell_conc, new_field = pl.pallas_call(
        functools.partial(place_kernel, blocks=blocks, cells=cells, subs=subs),
        out_shape=(f32((subs, blocks * cells)), f32(new.shape)),
        in_specs=[smem(), vmem(), vmem()],
        out_specs=(vmem(), vmem()),
        scratch_shapes=[pltpu.SMEM((slabs * CAP,), jnp.int32)],
        compiler_params=small(4),
        name="place",
    )(first.reshape(blocks), came.reshape(slabs * CAP * subs, cells), new)
    return (new_field.reshape(field.shape), cell_conc)


def solution(mesh):
    in_specs = (
        P("sa", ("grp", "gz"), "gy", None),
        P("sa"),
        P("sa", ("grp", "gz", "gy")),
        P("sa", ("grp", "gz", "gy")),
        P(("grp", "gz", "gy")),
        P(("grp", "gz", "gy"), None),
    )
    out_specs = (P("sa", ("grp", "gz"), "gy", None), P("sa", ("grp", "gz", "gy")))
    return jax.shard_map(shards, mesh=mesh, in_specs=in_specs, out_specs=out_specs, check_vma=False)
```

```python
import functools

import jax
import jax.numpy as jnp
from jax import lax
from jax.experimental import pallas as pl
from jax.experimental.pallas import tpu as pltpu
from jax.sharding import PartitionSpec as P

CAP = 6


def extended(x, sides, width):
    edges = {}
    for axis, dim in sides:
        size, length = (lax.axis_size(axis), x.shape[dim])
        up = [(i, (i + 1) % size) for i in range(size - 1)]
        last = lax.slice_in_dim(x, length - width, length, axis=dim)
        leading = lax.slice_in_dim(x, 0, width, axis=dim)
        edges[dim] = (
            lax.ppermute(last, axis, up),
            lax.ppermute(leading, axis, [(b, a) for a, b in up]),
        )
    done = []
    for _, dim in sides:
        low, high = edges[dim]
        around = [(width, width) if d in done else (0, 0) for d in range(x.ndim)]
        x = jnp.concatenate([jnp.pad(low, around), x, jnp.pad(high, around)], axis=dim)
        done.append(dim)
    return x


def neighbours(padded):
    beside_all = padded[:, 2:, 1:-1, 1:-1] + padded[:, :-2, 1:-1, 1:-1]
    beside_all = beside_all + padded[:, 1:-1, 2:, 1:-1] + padded[:, 1:-1, :-2, 1:-1]
    return beside_all + padded[:, 1:-1, 1:-1, 2:] + padded[:, 1:-1, 1:-1, :-2]


def diffuse(field, diffusion):
    padded = extended(field, (("gz", 1), ("gy", 2)), 1)
    padded = jnp.pad(padded, ((0, 0), (0, 0), (0, 0), (1, 1)))
    return field + diffusion[:, None, None, None] * (neighbours(padded) - 6.0 * field)


def rows_of(channels):
    return CAP * channels, CAP * channels + CAP


def pack_kernel(
    dest_in, secrete_in, uptake_in, voxel_in, out, dest, secrete, uptake, voxel, used, sems, *, slabs, subs
):
    pairs = ((dest_in, dest), (secrete_in, secrete), (uptake_in, uptake), (voxel_in, voxel))
    copies = [pltpu.make_async_copy(a, b, sems.at[i]) for i, (a, b) in enumerate(pairs)]
    for copy in copies:
        copy.start()
    cells = out.shape[1]
    base, rows = rows_of(2 * subs)
    for i in range(slabs):
        out[i * rows + base : (i + 1) * rows, :] = jnp.full((rows - base, cells), -1.0, jnp.float32)
        used[i] = 0
    for copy in copies:
        copy.wait()
    for b in range(dest.shape[0]):
        to = dest[b]
        slot = used[to]
        used[to] = slot + 1
        at = slice(b * cells, (b + 1) * cells)
        first = to * rows + slot * 2 * subs
        out[pl.ds(first, subs), :] = secrete[:, at]
        out[pl.ds(first + subs, subs), :] = uptake[:, at]
        out[pl.ds(to * rows + base + slot, 1), :] = voxel[b : b + 1, :].astype(jnp.float32)


def place_kernel(first, came, new, out, new_field, used, sem, *, blocks, cells, subs):
    leave = pltpu.make_async_copy(new, new_field, sem)
    leave.start()
    for i in range(0, came.shape[0] // subs, CAP):
        used[i] = i
    for b in range(blocks):
        slab = first[b]
        slot = used[slab]
        used[slab] = slot + 1
        out[:, b * cells : (b + 1) * cells] = came[pl.ds(slot * subs, subs), :]
    leave.wait()


def halves(x):
    high = x.astype(jnp.bfloat16)
    return high, (x - high.astype(jnp.float32)).astype(jnp.bfloat16)


SIZES, PART = (18, 34, 48, 96), 2
BITS = 10


def list_blocks(got, work, high_of, low_of, slabs, subs, highs):
    base, rows = rows_of(2 * subs)
    lanes = got.shape[1]
    lane_bits, high_bits = lanes.bit_length() - 1, highs.bit_length() - 1
    lane = lax.broadcasted_iota(jnp.int32, (CAP, lanes), 1)
    words, total, hole = [], jnp.int32(0), jnp.int32(0)
    for w in range(slabs // 8):
        marks = jnp.zeros((CAP, lanes), jnp.float32)
        for k in range(8):
            i = w * 8 + k
            v = got[i * rows + base : (i + 1) * rows, :].astype(jnp.int32)
            row = v >> lane_bits
            here = v >= 0
            high = jnp.where(here, row & (highs - 1), -1)
            low = (v & (lanes - 1)) | ((row >> high_bits) << lane_bits)
            high_of[i * CAP : (i + 1) * CAP, :] = high.astype(jnp.float32)
            low_of[i * CAP : (i + 1) * CAP, :] = low.astype(jnp.float32)
            marks = marks + jnp.where(here & (lane == 0), float(8**k), 0.0)
        words.append(jnp.sum(marks).astype(jnp.int32))
    for i in range(slabs):
        count = (words[i // 8] >> (3 * (i % 8))) & 7
        for slot in range(CAP):
            at = i * rows + slot * 2 * subs, i * CAP + slot, (i * CAP + slot) * subs
            code = at[0] | at[1] << BITS | at[2] << 2 * BITS
            work[total + slot] = code
        hole = jnp.where(count < CAP, code, hole)
        total = total + count
    for k in range(SIZES[-1] // 2):
        work[total + k] = hole
    return total


def spread_row(ref, row):
    own = ref[pl.ds(row, 8, stride=0), :]
    return jnp.concatenate([own, own], axis=0).astype(jnp.bfloat16)


def onehots_of(ids, lows, wide):
    tiles = []
    for t in range(0, wide, 16):
        own = ids[t : t + 16, :].astype(jnp.bfloat16)
        row = [jnp.where(own == low, jnp.bfloat16(1.0), jnp.bfloat16(0.0)) for low in lows]
        tiles.append(jnp.concatenate(row, axis=1))
    return jnp.concatenate(tiles, axis=0)


def cell_kernel(
    got, diffused, dest_in, new_out, back, dest_out, acc, table, ids, high_of, low_of, split, found, work, *, slabs, subs
):
    lanes = got.shape[1]
    channels = 2 * subs
    highs = diffused.shape[1] // 2
    wide = 2 * lanes
    mask = (1 << BITS) - 1
    total = list_blocks(got, work, high_of, low_of, slabs, subs, highs)
    ids[...] = lax.broadcasted_iota(jnp.int32, ids.shape, 0).astype(jnp.float32)

    def at_size(body):
        below = -1
        for size in SIZES:
            pl.when((total > below) & (total <= size))(functools.partial(body, size))
            below = size

    def add(size):
        partial = []
        first = ids[0:highs, :].astype(jnp.bfloat16)
        for p in range(0, size, PART):
            spreads, lows = [], []
            for k in range(p, p + PART):
                code = work[k]
                slot = (code >> BITS) & mask
                high, low = halves(got[pl.ds(code & mask, channels), :])
                at = k * 2 * channels
                split[at : at + channels, :] = high.astype(jnp.float32)
                split[at + channels : at + 2 * channels, :] = low.astype(jnp.float32)
                here = first == spread_row(high_of, slot)
                own = [jnp.where(here, spread_row(split, at + r), jnp.bfloat16(0.0)) for r in range(2 * channels)]
                spreads.append(jnp.concatenate(own, axis=0))
                lows.append(spread_row(low_of, slot))
            partial.append(
                lax.dot_general(
                    jnp.concatenate(spreads, axis=1),
                    onehots_of(ids, lows, wide),
                    (((1,), (1,)), ((), ())),
                    preferred_element_type=jnp.float32,
                )
            )
        acc[...] = sum(partial[1:], partial[0])

    at_size(add)
    half = channels * highs
    sums = (acc[0:half, :] + acc[half : 2 * half, :]).reshape(channels, highs, wide)
    sums = jnp.concatenate([sums[:, :, :lanes], sums[:, :, lanes:]], axis=1)
    new = (diffused[...] + sums[:subs]) / (1.0 + sums[subs:])
    new_out[...] = new
    dest_out[...] = dest_in[...]
    by_low = jnp.concatenate([new[:, :highs], new[:, highs:]], axis=2).reshape(subs * highs, wide)
    table[...] = jnp.concatenate([h.astype(jnp.float32) for h in halves(by_low)], axis=0)

    sub = lax.broadcasted_iota(jnp.int32, (8, lanes), 0)
    subf = sub.astype(jnp.float32)

    def read(size):
        values = table[...].astype(jnp.bfloat16)
        for p in range(0, size, PART):
            codes = [work[k] for k in range(p, p + PART)]
            slots = [(code >> BITS) & mask for code in codes]
            onehot = onehots_of(ids, [spread_row(low_of, slot) for slot in slots], wide)
            rows = jnp.dot(values, onehot, preferred_element_type=jnp.float32)
            rows = rows[: subs * highs] + rows[subs * highs :]
            for k in range(PART):
                own = rows[:, k * lanes : (k + 1) * lanes]
                high = high_of[pl.ds(slots[k], 8, stride=0), :]
                at = 8 * (p + k)
                found[at : at + 8, :] = found_rows(own, subf == high, subf + 8.0 == high, sub, subs, highs)
                back[pl.ds(codes[k] >> 2 * BITS, subs), :] = found[pl.ds(at + 1, subs, stride=2), :]

    at_size(read)


def found_rows(own, first, second, sub, subs, highs):
    assert subs == 4 and highs == 16
    fours = []
    for s in range(subs):
        a = own[s * highs : s * highs + 8, :]
        b = own[s * highs + 8 : s * highs + 16, :]
        x = jnp.where(first, a, jnp.where(second, b, 0.0))
        fours.append(x + pltpu.roll(x, 4, 0))
    upper = jnp.where(sub < 4, fours[1], fours[3])
    lower = jnp.where(sub < 4, fours[0], fours[2])
    upper = upper + pltpu.roll(upper, 2, 0)
    lower = lower + pltpu.roll(lower, 2, 0)
    both = jnp.where((sub & 2) == 2, upper, pltpu.roll(lower, 6, 0))
    return both + pltpu.roll(both, 1, 0)


def small(mebibytes):
    return pltpu.CompilerParams(vmem_limit_bytes=mebibytes << 20)


def vmem():
    return pl.BlockSpec(memory_space=pltpu.VMEM)


def smem():
    return pl.BlockSpec(memory_space=pltpu.SMEM)


def call_cells(got, diffused, dest, slabs, subs):
    lines, lanes = diffused.shape[1:]
    f32 = functools.partial(jax.ShapeDtypeStruct, dtype=jnp.float32)
    return pl.pallas_call(
        functools.partial(cell_kernel, slabs=slabs, subs=subs),
        out_shape=(f32((subs, lines, lanes)), f32((slabs * CAP * subs, lanes)), jax.ShapeDtypeStruct(dest.shape, dest.dtype)),
        in_specs=[vmem(), vmem(), vmem()],
        out_specs=(vmem(), vmem(), vmem()),
        scratch_shapes=[
            pltpu.VMEM((4 * subs * lines // 2, 2 * lanes), jnp.float32),
            pltpu.VMEM((2 * subs * lines // 2, 2 * lanes), jnp.float32),
            pltpu.VMEM((2 * lanes, lanes), jnp.float32),
            pltpu.VMEM((slabs * CAP, lanes), jnp.float32),
            pltpu.VMEM((slabs * CAP, lanes), jnp.float32),
            pltpu.VMEM((slabs * CAP * 4 * subs, lanes), jnp.float32),
            pltpu.VMEM((slabs * CAP * 8, lanes), jnp.float32),
            pltpu.SMEM((2 * slabs * CAP,), jnp.int32),
        ],
        compiler_params=small(8),
        name="cells",
    )(got, diffused, dest)


def shards(field, diffusion, secrete, uptake, cell_voxel, block_dest):
    subs, lanes = field.shape[0], field.shape[3]
    lines = field.shape[1] * field.shape[2]
    blocks = block_dest.shape[0]
    cells = secrete.shape[1] // blocks
    slabs = lax.axis_size("gz")
    base, rows = rows_of(2 * subs)
    f32 = functools.partial(jax.ShapeDtypeStruct, dtype=jnp.float32)
    dest = block_dest.reshape(blocks)
    sent = pl.pallas_call(
        functools.partial(pack_kernel, slabs=slabs, subs=subs),
        out_shape=f32((slabs * rows, cells)),
        in_specs=[pl.BlockSpec(memory_space=pltpu.HBM)] * 4,
        out_specs=vmem(),
        scratch_shapes=[
            pltpu.SMEM((blocks,), jnp.int32),
            pltpu.VMEM((subs, blocks * cells), jnp.float32),
            pltpu.VMEM((subs, blocks * cells), jnp.float32),
            pltpu.VMEM((blocks, cells), jnp.int32),
            pltpu.SMEM((slabs,), jnp.int32),
            pltpu.SemaphoreType.DMA((4,)),
        ],
        name="pack",
    )(dest, secrete, uptake, cell_voxel.reshape(blocks, cells))
    sent = sent.reshape(slabs, rows // 2, 2, cells)
    got = lax.all_to_all(sent, "gz", split_axis=0, concat_axis=0, tiled=True)
    diffused = diffuse(field, diffusion).reshape(subs, lines, lanes)
    new, back, first = call_cells(got.reshape(slabs * rows, cells), diffused, block_dest.reshape(1, blocks) * CAP, slabs, subs)
    back = back.reshape(slabs, CAP * subs, cells)
    came = lax.all_to_all(back, "gz", split_axis=0, concat_axis=0, tiled=True)
    cell_conc, new_field = pl.pallas_call(
        functools.partial(place_kernel, blocks=blocks, cells=cells, subs=subs),
        out_shape=(f32((subs, blocks * cells)), f32(new.shape)),
        in_specs=[smem(), vmem(), vmem()],
        out_specs=(vmem(), pl.BlockSpec(memory_space=pltpu.HBM)),
        scratch_shapes=[pltpu.SMEM((slabs * CAP,), jnp.int32), pltpu.SemaphoreType.DMA],
        compiler_params=small(4),
        name="place",
    )(first.reshape(blocks), came.reshape(slabs * CAP * subs, cells), new)
    return (new_field.reshape(field.shape), cell_conc)


def solution(mesh):
    in_specs = (
        P("sa", ("grp", "gz"), "gy", None),
        P("sa"),
        P("sa", ("grp", "gz", "gy")),
        P("sa", ("grp", "gz", "gy")),
        P(("grp", "gz", "gy")),
        P(("grp", "gz", "gy"), None),
    )
    out_specs = (P("sa", ("grp", "gz"), "gy", None), P("sa", ("grp", "gz", "gy")))
    return jax.shard_map(shards, mesh=mesh, in_specs=in_specs, out_specs=out_specs, check_vma=False)
```
